32 devices in a mesh: rec: 8 (over y, x, core), tile: 4 (over z).
Axes of the slice: x: 2, y: 2, z: 4, core: 2. Of those that a mesh axis runs over, the one named last changes fastest.
Arguments:
- deviation: float32 [64, 16, 512], P(None, 'rec', 'tile'), may hold values from -6 to 6
- footprint: bfloat16 [2048, 4, 2, 8, 8, 128], P('rec', 'tile'), may hold values from -0.046875 to 0.046875
- tile_list: int32 [2048, 4, 2], P('rec', 'tile'), may hold values from -1 to 1, as said below
- offset: int32 [2048], P('rec'), may hold values from 0 to 56
- observed: float32 [2048], P('rec'), may hold values from -10 to 10
- obs_group: int32 [2048], P('rec'), may hold values from 0 to 3
- group_var: float32 [4], replicated, may hold values from 0.5 to 4
- inv_time: float32 [64, 64], replicated, as said below
- inv_lat: float32 [16, 16], replicated, as said below
- inv_lon: float32 [512, 512], P('tile'), as said below
Outputs:
- gradient: float32 [64, 16, 512], P(None, 'rec', 'tile')
- misfit: float32 [2048], P('rec')
The draws below stay inside these ranges and needn't reach their ends.
Inputs may be any that keep to these rules, and one draw needn't show every extreme that they name: `tile_list`: each entry is a latitude tile of 8 rows in the slot's longitude strip, or -1 for an unused slot; the tiles named by one receptor in one strip are distinct. `inv_lon`: symmetric and diagonally dominant with a positive diagonal. `inv_lat`: symmetric and diagonally dominant with a positive diagonal. `inv_time`: symmetric and diagonally dominant with a positive diagonal.
All inputs are finite; a program needn't handle non-finite values.
Results may differ from the reference program's by a relative error of at most 0.0003.
Values sent between devices are 32-bit elements; how exact they have to be, the bound alone decides.
No kernel may reach another device: no remote copies, remote signals or barrier semaphores. Data moves between devices by JAX's collectives and lax.ppermute only.
A program may use at most 128 MiB of HBM per device.

```python
import math
import jax
import jax.numpy as jnp
from jax import lax

P_SIZE = 64
W = 8
TY = 8
K = 2
GROUPS = 4
LON_DEV = 128
REC_DEV = 256
NY = 16
NX = 512
RECEPTORS = 2048
N_REC = 8
N_TILE = 4


def draw_square(key, matrix_order):
    key_one, key_two = jax.random.split(key)
    entries = jax.random.normal(key_one, (matrix_order, matrix_order), jnp.float32)
    entries = entries * (0.8 / matrix_order)
    symmetric = (entries + entries.T) * 0.5
    identity_mat = jnp.eye(matrix_order, dtype=jnp.float32)
    off_diag = symmetric * (1.0 - identity_mat)
    baseline = jax.random.uniform(key_two, (matrix_order,), jnp.float32, 0.5, 1.5)
    diagonal_vals = baseline + jnp.sum(jnp.abs(off_diag), axis=1)
    return off_diag + identity_mat * diagonal_vals[:, None]


def draw_inv_time(key, part):
    return draw_square(jax.random.fold_in(key, 11), P_SIZE)


def draw_inv_lat(key, part):
    return draw_square(jax.random.fold_in(key, 12), NY)


def draw_inv_lon(key, part):
    return draw_square(jax.random.fold_in(key, 13), NX)


def draw_tile_list(key, part):
    tiles_y = NY // TY
    key_one, key_two, key_three = jax.random.split(jax.random.fold_in(key, 14), 3)
    scores = jax.random.randint(key_one, (RECEPTORS, N_TILE, tiles_y), 0, 65536) * tiles_y + jnp.arange(tiles_y, dtype=jnp.int32)
    ranking = jnp.argsort(scores, axis=-1).astype(jnp.int32)[..., :K]
    strip_level = jax.random.randint(key_two, (1, N_TILE, 1), 0, K + 1)
    receptor_extra = jax.random.randint(key_three, (RECEPTORS, N_TILE, 1), 0, K + 1)
    used_count = jnp.minimum(strip_level + receptor_extra, K)
    slot_pos = jnp.arange(K, dtype=jnp.int32)[None, None, :]
    return jnp.where(slot_pos < used_count, ranking, -1).astype(jnp.int32)


def set_ends(drawn, own_key, low, high):
    extent = drawn.shape
    spot = [jax.random.randint(jax.random.fold_in(own_key, axis), (), 0, extent[axis]) for axis in range(len(extent))]
    drawn = drawn.at[tuple(spot)].set(low)
    longest = extent.index(max(extent))
    spot[longest] = (spot[longest] + 1) % extent[longest]
    return drawn.at[tuple(spot)].set(high)


def block_scale(own_key, dims, pieces, smallest, top_value):
    def one(dim, parts):
        heights = jax.random.uniform(jax.random.fold_in(jax.random.fold_in(own_key, 6), dim), (parts,), jnp.float32, smallest / len(pieces), top_value / len(pieces))
        return jnp.repeat(jnp.exp(heights), dims[dim] // parts).reshape((-1,) + (1,) * (len(dims) - dim - 1))

    factor_of = one(*pieces[0])
    for cut in pieces[1:]:
        factor_of = factor_of * one(*cut)
    return factor_of


def noise(own_key, dims, scale, limit, pieces=(), kind=jnp.bfloat16):
    level = block_scale(own_key, dims, pieces, -0.22, 0.18) if pieces else 1.0
    values = jax.random.normal(own_key, dims, jnp.float32) * scale * level
    return jnp.minimum(jnp.maximum(values, -limit), limit).astype(kind)


def setup_inputs(seed: int = 0) -> dict:
    keys = jax.random.split(jax.random.key(seed), 11)
    deviation = noise(keys[0], (P_SIZE, NY, NX), 1.0, 6.0, ((1, 8), (2, 4)), jnp.float32)
    footprint = noise(keys[1], (RECEPTORS, N_TILE, K, W, TY, LON_DEV), (K * W * TY * LON_DEV) ** -0.5, 0.046875, ((0, 8), (1, 4)))
    tile_list = draw_tile_list(jax.random.fold_in(keys[10], 71), 0)
    offset = set_ends(jax.random.randint(keys[3], (RECEPTORS,), 0, P_SIZE - W + 1), jax.random.fold_in(keys[3], 1), 0, P_SIZE - W).astype(jnp.int32)
    observed = noise(keys[4], (RECEPTORS,), 2.0, 10.0, ((0, 8),), jnp.float32)
    obs_group = set_ends(jax.random.randint(keys[5], (RECEPTORS,), 0, GROUPS), jax.random.fold_in(keys[5], 1), 0, GROUPS - 1).astype(jnp.int32)
    group_var = jnp.clip(jnp.exp(jax.random.uniform(keys[6], (GROUPS,), jnp.float32, math.log(0.5), math.log(4.0))), 0.5, 4.0)
    inv_time = draw_inv_time(jax.random.fold_in(keys[10], 71), 0)
    inv_lat = draw_inv_lat(jax.random.fold_in(keys[10], 71), 0)
    inv_lon = draw_inv_lon(jax.random.fold_in(keys[10], 71), 0)
    return dict(deviation=deviation, footprint=footprint, tile_list=tile_list, offset=offset, observed=observed, obs_group=obs_group, group_var=group_var, inv_time=inv_time, inv_lat=inv_lat, inv_lon=inv_lon)


def reference(deviation, footprint, tile_list, offset, observed, obs_group, group_var, inv_time, inv_lat, inv_lon):
    highest = lax.Precision.HIGHEST
    tiles_y = NY // TY
    tile_cells = TY * LON_DEV
    strips = deviation.reshape(P_SIZE, NY, N_TILE, LON_DEV).transpose(2, 0, 1, 3).reshape(N_TILE, P_SIZE * tiles_y, tile_cells)
    active = (tile_list >= 0).astype(jnp.float32)
    starts = offset[:, None] + jnp.arange(W, dtype=jnp.int32)[None, :]
    row_index = (starts[:, None, None, :] * tiles_y + jnp.maximum(tile_list, 0)[:, :, :, None]).astype(jnp.int32)
    groups_foot = footprint.reshape(N_REC, REC_DEV, N_TILE, K, W, tile_cells)
    groups_index = row_index.reshape(N_REC, REC_DEV, N_TILE, K, W)
    groups_active = active.reshape(N_REC, REC_DEV, N_TILE, K)
    strip_ids = jnp.arange(N_TILE, dtype=jnp.int32)[None, :, None, None]

    def forward(element):
        foot_block, row_ids, active_slots = element
        picked = strips[strip_ids, row_ids]
        products = jnp.sum(foot_block.astype(jnp.float32) * picked, axis=(3, 4))
        return jnp.sum(products * active_slots, axis=(1, 2))

    predicted = lax.map(forward, (groups_foot, groups_index, groups_active)).reshape(RECEPTORS)
    variance = group_var[obs_group]
    misfit = (predicted - observed) / variance
    groups_weight = misfit.reshape(N_REC, REC_DEV)[:, :, None, None] * groups_active

    def adjoint(running, element):
        foot_block, row_ids, slot_weight = element
        contrib = foot_block.astype(jnp.float32) * slot_weight[:, :, :, None, None]
        running = running.at[strip_ids, row_ids].add(contrib)
        return running, None

    start_sum = jnp.zeros((N_TILE, P_SIZE * tiles_y, tile_cells), jnp.float32)
    summed, _ = lax.scan(adjoint, start_sum, (groups_foot, groups_index, groups_weight))
    adjoint_field = summed.reshape(N_TILE, P_SIZE, NY, LON_DEV).transpose(1, 2, 0, 3).reshape(P_SIZE, NY, NX)
    lat_done = jnp.einsum("an,pnm->pam", inv_lat, deviation, precision=highest)
    lon_done = jnp.einsum("pam,cm->pac", lat_done, inv_lon, precision=highest)
    time_done = jnp.einsum("qp,pac->qac", inv_time, lon_done, precision=highest)
    return time_done + adjoint_field, misfit
```

```python
import functools

import jax
import jax.numpy as jnp
from jax import lax
from jax.experimental import pallas as pl
from jax.experimental.pallas import tpu as pltpu
from jax.sharding import PartitionSpec as P

GROUP = 8
HIGHEST = lax.Precision.HIGHEST


def place(owner, lat_dev, tile_rows):
    row = owner * lat_dev
    return row // tile_rows, lax.rem(row, tile_rows)


def forward_kernel(dims, tile_ref, offset_ref, own_ref, foot_ref, *refs):
    periods, tiles_y, tile_rows, lat_dev, receptors, slots, window = dims
    blocks = refs[:-3]
    out_ref, table, sums = refs[-3:]
    lanes = table.shape[-1]
    for dist, block in enumerate(blocks):
        tile, row = place(own_ref[0] ^ dist, lat_dev, tile_rows)
        table[tile, :, pl.ds(row, lat_dev), :] = block[...]
    table[tiles_y] = jnp.zeros(table.shape[1:], jnp.float32)

    def step(group, carry):
        for item in range(GROUP):
            receptor = group * GROUP + item
            start = offset_ref[receptor]
            total = None
            for slot in range(slots):
                tile = tile_ref[slot, receptor]
                tile = jnp.where(tile < 0, tiles_y, tile)
                field = table[tile, pl.ds(start, window)]
                block = foot_ref[receptor, slot].astype(jnp.float32)
                part = jnp.sum(block * field, axis=0)
                total = part if total is None else total + part
            sums[receptor] = total
        return carry

    lax.fori_loop(0, receptors // GROUP, step, 0)
    rows = jnp.sum(sums[...], axis=1)
    ones = jnp.ones((8, lanes), jnp.float32)
    flat = lax.dot_general(
        ones,
        rows,
        (((1,), (1,)), ((), ())),
        precision=HIGHEST,
        preferred_element_type=jnp.float32,
    )
    out_ref[...] = flat[0:1, :]


def adjoint_kernel(dims, n_tile, tile_ref, offset_ref, own_ref, var_ref, foot_ref, *refs):
    periods, tiles_y, tile_rows, lat_dev, receptors, slots, window = dims
    preds = refs[:n_tile]
    observed_ref, group_ref, field_ref, lat_ref = refs[n_tile : n_tile + 4]
    n_rec = (tiles_y * tile_rows) // lat_dev
    outs = refs[n_tile + 4 : n_tile + 4 + n_rec]
    misfit_ref = refs[n_tile + 4 + n_rec]
    weight = refs[n_tile + 5 + n_rec]
    accs = refs[n_tile + 6 + n_rec :]
    lanes = weight.shape[-1]
    predicted = preds[0][...]
    for other in preds[1:]:
        predicted = predicted + other[...]
    group = group_ref[...]
    variance = jnp.zeros(group.shape, jnp.float32)
    for index in range(var_ref.shape[0]):
        variance = jnp.where(group == index, var_ref[index], variance)
    misfit = (predicted - observed_ref[...]) / variance
    misfit_ref[...] = misfit
    weight[...] = jnp.transpose(jnp.broadcast_to(misfit, (lanes, receptors)))
    for acc in accs:
        acc[...] = jnp.zeros(acc.shape, jnp.float32)

    def step(group, carry):
        for item in range(GROUP):
            receptor = group * GROUP + item
            start = offset_ref[receptor]
            scale = jnp.broadcast_to(weight[pl.ds(receptor, 1), :], (tile_rows, lanes))
            for slot in range(slots):
                tile = tile_ref[slot, receptor]
                tile = jnp.where(tile < 0, tiles_y, tile)
                acc = accs[(item * slots + slot) % len(accs)]
                block = foot_ref[receptor, slot].astype(jnp.float32)
                acc[tile, pl.ds(start, window)] += block * scale[None]
        return carry

    lax.fori_loop(0, receptors // GROUP, step, 0)
    total = accs[0]

    def finish(period, carry):
        for tile in range(tiles_y):
            value = total[tile, period]
            for acc in accs[1:]:
                value = value + acc[tile, period]
            for row in range(lat_dev):
                line = jnp.broadcast_to(field_ref[period, pl.ds(row, 1), :], (tile_rows, lanes))
                value = value + lat_ref[row, pl.ds(tile * tile_rows, tile_rows), :] * line
            total[tile, period] = value
        return carry

    lax.fori_loop(0, periods, finish, 0, unroll=4)
    for dist, out in enumerate(outs):
        tile, row = place(own_ref[0] ^ dist, lat_dev, tile_rows)
        out[...] = total[tile, :, pl.ds(row, lat_dev), :]


def shards(
    deviation,
    footprint,
    tile_list,
    offset,
    observed,
    obs_group,
    group_var,
    inv_time,
    inv_lat,
    inv_lon,
):
    periods, lat_dev, lon_dev = deviation.shape
    receptors, _, slots, window, tile_rows, _ = footprint.shape
    n_rec = lax.axis_size("rec")
    n_tile = lax.axis_size("tile")
    tiles_y = lat_dev * n_rec // tile_rows
    dims = (periods, tiles_y, tile_rows, lat_dev, receptors, slots, window)
    own = lax.axis_index("rec")

    def swap(value, axis, dist):
        size = lax.axis_size(axis)
        return lax.ppermute(value, axis, [(i, i ^ dist) for i in range(size)])

    even = [deviation] + [swap(deviation, "rec", d) for d in range(2, n_rec, 2)]
    odd = [swap(value, "rec", 1) for value in even]
    blocks = [value for pair in zip(even, odd) for value in pair]
    strips = [deviation] + [swap(deviation, "tile", d) for d in range(1, n_tile)]

    tiles = tile_list[:, 0, :].T
    foot = footprint[:, 0]
    own_arr = own.reshape(1)
    smem = pl.BlockSpec(memory_space=pltpu.SMEM)
    vmem = pl.BlockSpec(memory_space=pltpu.VMEM)
    block_shape = jax.ShapeDtypeStruct((periods, lat_dev, lon_dev), jnp.float32)
    line_shape = jax.ShapeDtypeStruct((1, receptors), jnp.float32)
    table_shape = pltpu.VMEM((tiles_y + 1, periods, tile_rows, lon_dev), jnp.float32)
    params = pltpu.CompilerParams(vmem_limit_bytes=32 * 2**20)
    partial_pred = pl.pallas_call(
        functools.partial(forward_kernel, dims),
        out_shape=line_shape,
        in_specs=[smem] * 3 + [vmem] * (1 + n_rec),
        out_specs=vmem,
        scratch_shapes=[table_shape, pltpu.VMEM((receptors, tile_rows, lon_dev), jnp.float32)],
        compiler_params=params,
    )(tiles, offset, own_arr, foot, *blocks)
    preds = [partial_pred] + [swap(partial_pred, "tile", d) for d in range(1, n_tile)]

    strip = lax.axis_index("tile")
    lon_done = None
    for dist, value in enumerate(strips):
        part = lax.dynamic_slice_in_dim(inv_lon, (strip ^ dist) * lon_dev, lon_dev, 1)
        term = jnp.einsum("pnm,cm->pnc", value, part, precision=HIGHEST)
        lon_done = term if lon_done is None else lon_done + term
    field = jnp.einsum("qp,pnc->qnc", inv_time, lon_done, precision=HIGHEST)
    own_lat = lax.dynamic_slice_in_dim(inv_lat, own * lat_dev, lat_dev, 1)
    lat_cols = jnp.broadcast_to(own_lat.T[:, :, None], (lat_dev, tiles_y * tile_rows, lon_dev))

    n_acc = 4
    results = pl.pallas_call(
        functools.partial(adjoint_kernel, dims, n_tile),
        out_shape=[block_shape] * n_rec + [line_shape],
        in_specs=[smem] * 4 + [vmem] * (1 + n_tile + 4),
        out_specs=[vmem] * (n_rec + 1),
        scratch_shapes=[pltpu.VMEM((receptors, lon_dev), jnp.float32)] + [table_shape] * n_acc,
        compiler_params=params,
    )(
        tiles,
        offset,
        own_arr,
        group_var,
        foot,
        *preds,
        observed.reshape(1, receptors),
        obs_group.reshape(1, receptors),
        field,
        lat_cols,
    )
    misfit = results[n_rec].reshape(receptors)
    summed = [results[d] + swap(results[d + 1], "rec", 1) for d in range(0, n_rec, 2)]
    gradient = summed[0]
    for index in range(1, n_rec // 2):
        gradient = gradient + swap(summed[index], "rec", 2 * index)
    return (gradient, misfit)


def solution(mesh):
    return jax.shard_map(
        shards,
        mesh=mesh,
        in_specs=(
            P(None, "rec", "tile"),
            P("rec", "tile", None, None, None, None),
            P("rec", "tile", None),
            P("rec"),
            P("rec"),
            P("rec"),
            P(),
            P(),
            P(),
            P("tile", None),
        ),
        out_specs=(P(None, "rec", "tile"), P("rec")),
        check_vma=False,
    )
```

```python
import functools

import jax
import jax.numpy as jnp
from jax import lax
from jax.experimental import pallas as pl
from jax.experimental.pallas import tpu as pltpu
from jax.sharding import PartitionSpec as P


GROUP = 8
N_ACC = 4
CHUNKS = 8
HIGHEST = lax.Precision.HIGHEST


def dot(left, right, dims=((1,), (0,))):
    return lax.dot_general(
        left, right, (dims, ((), ())), precision=HIGHEST, preferred_element_type=jnp.float32
    )


def place(owner, dims):
    periods, _, tile_rows, lat_dev = dims[:4]
    row = owner * lat_dev
    return (row // tile_rows) * (periods * tile_rows) + lax.rem(row, tile_rows)


def index_kernel(dims, tile_hbm, offset_hbm, base_ref, tile_ref, offset_ref, sems):
    periods, tiles_y = dims[:2]
    copies = [
        pltpu.make_async_copy(tile_hbm, tile_ref, sems.at[0]),
        pltpu.make_async_copy(offset_hbm, offset_ref, sems.at[1]),
    ]
    for copy in copies:
        copy.start()
    for copy in copies:
        copy.wait()
    tile = tile_ref[...]
    tile = jnp.where(tile < 0, tiles_y, tile)
    base_ref[...] = tile * periods + offset_ref[...]


def load_copies(base_ref, base, base_sem, foot_hbm, foot, foot_sems):
    chunk = foot.shape[0] // CHUNKS
    first = pltpu.make_async_copy(base_ref, base, base_sem)
    rest = [
        pltpu.make_async_copy(
            foot_hbm.at[pl.ds(index * chunk, chunk)],
            foot.at[pl.ds(index * chunk, chunk)],
            foot_sems.at[index],
        )
        for index in range(CHUNKS)
    ]
    first.start()
    for copy in rest:
        copy.start()
    return first, rest


def forward_kernel(dims, base_ref, foot_hbm, *refs):
    periods, tiles_y, tile_rows, lat_dev, receptors, slots, window = dims
    blocks = refs[:-7]
    out_ref, table, sums, base, base_sem, foot_ref, foot_sems = refs[-7:]
    lanes = table.shape[-1]
    first, rest_copies = load_copies(base_ref, base, base_sem, foot_hbm, foot_ref, foot_sems)
    own = lax.axis_index("rec")
    for dist, block in enumerate(blocks):
        start = place(own ^ dist, dims)
        for row in range(lat_dev):
            table[pl.ds(start + row, periods, stride=tile_rows), :] = block[
                pl.ds(row, periods, stride=lat_dev), :
            ]
    rest = tiles_y * periods * tile_rows
    table[pl.ds(rest, periods * tile_rows), :] = jnp.zeros((periods * tile_rows, lanes), jnp.float32)

    def step(group, carry):
        for item in range(GROUP):
            receptor = group * GROUP + item
            total = None
            for slot in range(slots):
                start = pl.multiple_of(base[slot, receptor] * tile_rows, tile_rows)
                field = table[pl.ds(start, window * tile_rows), :]
                field = field.reshape(window, tile_rows, lanes)
                block = foot_ref[receptor, slot].astype(jnp.float32)
                part = jnp.sum(block * field, axis=0)
                total = part if total is None else total + part
            sums[receptor] = total
        return carry

    first.wait()
    groups = receptors // GROUP // CHUNKS
    for index, copy in enumerate(rest_copies):
        copy.wait()
        lax.fori_loop(index * groups, (index + 1) * groups, step, 0)
    rows = jnp.sum(sums[...], axis=1)
    flat = dot(jnp.ones((8, lanes), jnp.float32), rows, ((1,), (1,)))
    out_ref[...] = flat[0:1, :]


def prior_kernel(dims, n_tile, *refs):
    periods, tiles_y, tile_rows, lat_dev = dims[:4]
    own, strip = lax.axis_index("rec"), lax.axis_index("tile")
    strips = refs[:n_tile]
    lon_ref, time_ref, lat_ref, out_ref, mixed = refs[n_tile:]
    lanes = out_ref.shape[-1]
    total = None
    for dist, value in enumerate(strips):
        start = pl.multiple_of((strip ^ dist) * lanes, lanes)
        term = dot(value[...], lon_ref[:, pl.ds(start, lanes)], ((1,), (1,)))
        total = term if total is None else total + term
    mixed[...] = total
    fields = [
        dot(time_ref[...], mixed[pl.ds(row, periods, stride=lat_dev), :]) for row in range(lat_dev)
    ]
    for row in range(lat_dev):
        mixed[pl.ds(row * periods, periods), :] = fields[row]
    cols = [lat_ref[pl.ds(own * lat_dev + row, 1), :] for row in range(lat_dev)]
    cols = [
        jnp.transpose(jnp.broadcast_to(col, (lanes, col.shape[-1]))) for col in cols
    ]

    def finish(period, carry):
        lines = [
            jnp.broadcast_to(mixed[pl.ds(row * periods + period, 1), :], (tile_rows, lanes))
            for row in range(lat_dev)
        ]
        for tile in range(tiles_y):
            value = None
            for row in range(lat_dev):
                term = cols[row][tile * tile_rows : (tile + 1) * tile_rows] * lines[row]
                value = term if value is None else value + term
            start = pl.multiple_of((tile * periods + period) * tile_rows, tile_rows)
            out_ref[pl.ds(start, tile_rows), :] = value
        return carry

    lax.fori_loop(0, periods, finish, 0, unroll=8)


def adjoint_kernel(dims, n_tile, base_ref, foot_hbm, *refs):
    periods, tiles_y, tile_rows, lat_dev, receptors, slots, window = dims
    preds = refs[:n_tile]
    observed_ref, group_ref, var_ref, prior_ref = refs[n_tile : n_tile + 4]
    n_rec = (tiles_y * tile_rows) // lat_dev
    outs = refs[n_tile + 4 : n_tile + 4 + n_rec]
    scratch = refs[n_tile + 4 + n_rec :]
    misfit_ref, weight, base, base_sem, foot_ref, foot_sems = scratch[:6]
    accs = scratch[6:]
    lanes = weight.shape[-1]
    first, rest_copies = load_copies(base_ref, base, base_sem, foot_hbm, foot_ref, foot_sems)
    own = lax.axis_index("rec")
    predicted = preds[0][...]
    for other in preds[1:]:
        predicted = predicted + other[...]
    group = group_ref[...]
    variance = jnp.zeros(group.shape, jnp.float32)
    for index in range(var_ref.shape[1]):
        variance = jnp.where(group == index, var_ref[:, index : index + 1], variance)
    misfit = (predicted - observed_ref[...]) / variance
    misfit_ref[...] = misfit
    weight[...] = jnp.transpose(jnp.broadcast_to(misfit, (lanes, receptors)))
    for acc in accs:
        acc[...] = jnp.zeros(acc.shape, jnp.float32)

    def step(group, carry):
        for item in range(GROUP):
            receptor = group * GROUP + item
            scale = jnp.broadcast_to(weight[pl.ds(receptor, 1), :], (tile_rows, lanes))
            for slot in range(slots):
                start = pl.multiple_of(base[slot, receptor] * tile_rows, tile_rows)
                acc = accs[(item * slots + slot) % len(accs)]
                block = foot_ref[receptor, slot].astype(jnp.float32) * scale[None]
                acc[pl.ds(start, window * tile_rows), :] += block.reshape(window * tile_rows, lanes)
        return carry

    first.wait()
    groups = receptors // GROUP // CHUNKS
    for index, copy in enumerate(rest_copies):
        copy.wait()
        lax.fori_loop(index * groups, (index + 1) * groups, step, 0)
    total = accs[0]
    size = tiles_y * periods * tile_rows
    chunk = 8 * tile_rows

    def finish(index, carry):
        rows = pl.ds(pl.multiple_of(index * chunk, chunk), chunk)
        value = prior_ref[rows, :]
        for acc in accs:
            value = value + acc[rows, :]
        total[rows, :] = value
        return carry

    lax.fori_loop(0, size // chunk, finish, 0)
    for dist, out in enumerate(outs):
        start = place(own ^ dist, dims)
        for row in range(lat_dev):
            out[pl.ds(row, periods, stride=lat_dev), :] = total[
                pl.ds(start + row, periods, stride=tile_rows), :
            ]


def shards(
    deviation,
    footprint,
    tile_list,
    offset,
    observed,
    obs_group,
    group_var,
    inv_time,
    inv_lat,
    inv_lon,
):
    periods, lat_dev, lon_dev = deviation.shape
    receptors, _, slots, window, tile_rows, _ = footprint.shape
    n_rec = lax.axis_size("rec")
    n_tile = lax.axis_size("tile")
    tiles_y = lat_dev * n_rec // tile_rows
    dims = (periods, tiles_y, tile_rows, lat_dev, receptors, slots, window)
    anywhere = pl.BlockSpec(memory_space=pltpu.HBM)
    vmem = pl.BlockSpec(memory_space=pltpu.VMEM)
    params = pltpu.CompilerParams(vmem_limit_bytes=48 * 2**20)
    field_rows = periods * lat_dev
    block_shape = jax.ShapeDtypeStruct((field_rows, lon_dev), jnp.float32)
    line_shape = jax.ShapeDtypeStruct((1, receptors), jnp.float32)
    prior_shape = jax.ShapeDtypeStruct((tiles_y * periods * tile_rows, lon_dev), jnp.float32)
    table_shape = pltpu.VMEM(((tiles_y + 1) * periods * tile_rows, lon_dev), jnp.float32)

    load_shapes = [
        pltpu.SMEM((slots, receptors), jnp.int32),
        pltpu.SemaphoreType.DMA,
        pltpu.VMEM((receptors, slots, window, tile_rows, lon_dev), footprint.dtype),
        pltpu.SemaphoreType.DMA((CHUNKS,)),
    ]

    def swap(value, axis, dist):
        size = lax.axis_size(axis)
        return lax.ppermute(value, axis, [(i, i ^ dist) for i in range(size)])

    local = deviation.reshape(field_rows, lon_dev)
    far = range(2, n_rec, 2)
    even = {0: local}
    for dist in far:
        even[dist] = swap(local, "rec", dist)
    blocks = []
    for dist in range(0, n_rec, 2):
        blocks += [even[dist], swap(even[dist], "rec", 1)]
    strips = [local] + [swap(local, "tile", d) for d in range(1, n_tile)]

    base = pl.pallas_call(
        functools.partial(index_kernel, dims),
        out_shape=jax.ShapeDtypeStruct((slots, receptors), jnp.int32),
        in_specs=[anywhere] * 2,
        out_specs=vmem,
        scratch_shapes=[
            pltpu.VMEM((slots, receptors), jnp.int32),
            pltpu.VMEM((1, receptors), jnp.int32),
            pltpu.SemaphoreType.DMA((2,)),
        ],
        compiler_params=pltpu.CompilerParams(vmem_limit_bytes=2**20),
        cost_estimate=pl.CostEstimate(flops=10**10, bytes_accessed=2 * 10**7, transcendentals=0),
    )(tile_list[:, 0, :].T, offset.reshape(1, receptors))
    foot = footprint[:, 0]
    partial_pred = pl.pallas_call(
        functools.partial(forward_kernel, dims),
        out_shape=line_shape,
        in_specs=[vmem, anywhere] + [vmem] * n_rec,
        out_specs=vmem,
        scratch_shapes=[table_shape, pltpu.VMEM((receptors, tile_rows, lon_dev), jnp.float32)]
        + load_shapes,
        compiler_params=params,
    )(base, foot, *blocks)
    preds = [partial_pred] + [swap(partial_pred, "tile", d) for d in range(1, n_tile)]
    prior = pl.pallas_call(
        functools.partial(prior_kernel, dims, n_tile),
        out_shape=prior_shape,
        in_specs=[vmem] * (n_tile + 3),
        out_specs=vmem,
        scratch_shapes=[pltpu.VMEM((field_rows, lon_dev), jnp.float32)],
        compiler_params=params,
    )(*strips, inv_lon, inv_time, inv_lat)
    results = pl.pallas_call(
        functools.partial(adjoint_kernel, dims, n_tile),
        out_shape=[block_shape] * n_rec + [line_shape],
        in_specs=[vmem, anywhere] + [vmem] * (n_tile + 4),
        out_specs=[vmem] * (n_rec + 1),
        scratch_shapes=[pltpu.VMEM((receptors, lon_dev), jnp.float32)]
        + load_shapes
        + [table_shape] * N_ACC,
        compiler_params=params,
    )(
        base,
        foot,
        *preds,
        observed.reshape(1, receptors),
        obs_group.reshape(1, receptors),
        group_var.reshape(1, -1),
        prior,
    )
    misfit = results[n_rec].reshape(receptors)
    gradient = None
    for dist in list(reversed(range(2, n_rec, 2))) + [0]:
        value = results[dist] + swap(results[dist + 1], "rec", 1)
        value = value if dist == 0 else swap(value, "rec", dist)
        gradient = value if gradient is None else gradient + value
    return (gradient.reshape(periods, lat_dev, lon_dev), misfit)


def solution(mesh):
    return jax.shard_map(
        shards,
        mesh=mesh,
        in_specs=(
            P(None, "rec", "tile"),
            P("rec", "tile", None, None, None, None),
            P("rec", "tile", None),
            P("rec"),
            P("rec"),
            P("rec"),
            P(),
            P(),
            P(),
            P("tile", None),
        ),
        out_specs=(P(None, "rec", "tile"), P("rec")),
        check_vma=False,
    )
```

```python
import functools

import jax
import jax.numpy as jnp
from jax import lax
from jax.experimental import pallas as pl
from jax.experimental.pallas import tpu as pltpu
from jax.sharding import PartitionSpec as P


GROUP = 8
N_ACC = 4
HIGHEST = lax.Precision.HIGHEST


def dot(left, right, dims=((1,), (0,))):
    return lax.dot_general(
        left, right, (dims, ((), ())), precision=HIGHEST, preferred_element_type=jnp.float32
    )


def place(owner, dims):
    periods, _, tile_rows, lat_dev = dims[:4]
    row = owner * lat_dev
    return (row // tile_rows) * (periods * tile_rows) + lax.rem(row, tile_rows)


def ones_kernel(ones_ref):
    ones_ref[...] = jnp.ones(ones_ref.shape, jnp.float32)


def window_start(dims, tile_ref, offset_ref, slot, receptor):
    periods, tiles_y, tile_rows = dims[:3]
    tile = tile_ref[slot, receptor]
    tile = jnp.where(tile < 0, tiles_y, tile)
    return pl.multiple_of((tile * periods + offset_ref[receptor]) * tile_rows, tile_rows)


def forward_kernel(dims, tile_ref, offset_ref, *refs):
    periods, tiles_y, tile_rows, lat_dev, receptors, slots, window = dims
    foot_ref, ones_ref, blocks = refs[0], refs[1], refs[2:-3]
    out_ref, table, sums = refs[-3:]
    lanes = table.shape[-1]
    own = lax.axis_index("rec")
    for dist, block in enumerate(blocks):
        start = place(own ^ dist, dims)
        for row in range(lat_dev):
            table[pl.ds(start + row, periods, stride=tile_rows), :] = block[
                pl.ds(row, periods, stride=lat_dev), :
            ]
    rest = tiles_y * periods * tile_rows
    table[pl.ds(rest, periods * tile_rows), :] = jnp.zeros((periods * tile_rows, lanes), jnp.float32)

    def step(group, carry):
        for item in range(GROUP):
            receptor = group * GROUP + item
            total = None
            for slot in range(slots):
                start = window_start(dims, tile_ref, offset_ref, slot, receptor)
                field = table[pl.ds(start, window * tile_rows), :]
                field = field.reshape(window, tile_rows, lanes)
                block = foot_ref[receptor, slot].astype(jnp.float32)
                part = jnp.sum(block * field, axis=0)
                total = part if total is None else total + part
            sums[receptor] = total
        return carry

    lax.fori_loop(0, receptors // GROUP, step, 0)
    rows = jnp.sum(sums[...], axis=1)
    flat = dot(ones_ref[...], rows, ((1,), (1,)))
    out_ref[...] = flat[0:1, :]


def prior_kernel(dims, n_tile, *refs):
    periods, tiles_y, tile_rows, lat_dev = dims[:4]
    own, strip = lax.axis_index("rec"), lax.axis_index("tile")
    strips = refs[:n_tile]
    lon_ref, time_ref, lat_ref, out_ref, mixed = refs[n_tile:]
    lanes = out_ref.shape[-1]
    total = None
    for dist, value in enumerate(strips):
        start = pl.multiple_of((strip ^ dist) * lanes, lanes)
        term = dot(value[...], lon_ref[:, pl.ds(start, lanes)], ((1,), (1,)))
        total = term if total is None else total + term
    mixed[...] = total
    fields = [
        dot(time_ref[...], mixed[pl.ds(row, periods, stride=lat_dev), :]) for row in range(lat_dev)
    ]
    for row in range(lat_dev):
        mixed[pl.ds(row * periods, periods), :] = fields[row]
    cols = [lat_ref[pl.ds(own * lat_dev + row, 1), :] for row in range(lat_dev)]
    cols = [
        jnp.transpose(jnp.broadcast_to(col, (lanes, col.shape[-1]))) for col in cols
    ]

    def finish(period, carry):
        lines = [
            jnp.broadcast_to(mixed[pl.ds(row * periods + period, 1), :], (tile_rows, lanes))
            for row in range(lat_dev)
        ]
        for tile in range(tiles_y):
            value = None
            for row in range(lat_dev):
                term = cols[row][tile * tile_rows : (tile + 1) * tile_rows] * lines[row]
                value = term if value is None else value + term
            start = pl.multiple_of((tile * periods + period) * tile_rows, tile_rows)
            out_ref[pl.ds(start, tile_rows), :] = value
        return carry

    lax.fori_loop(0, periods, finish, 0, unroll=8)


def adjoint_kernel(dims, n_tile, tile_ref, offset_ref, *refs):
    periods, tiles_y, tile_rows, lat_dev, receptors, slots, window = dims
    foot_ref, refs = refs[0], refs[1:]
    preds = refs[:n_tile]
    observed_ref, group_ref, var_ref, prior_ref = refs[n_tile : n_tile + 4]
    n_rec = (tiles_y * tile_rows) // lat_dev
    outs = refs[n_tile + 4 : n_tile + 4 + n_rec]
    scratch = refs[n_tile + 4 + n_rec :]
    misfit_ref, weight = scratch[:2]
    accs = scratch[2:]
    lanes = weight.shape[-1]
    own = lax.axis_index("rec")
    predicted = preds[0][...]
    for other in preds[1:]:
        predicted = predicted + other[...]
    group = group_ref[...]
    variance = jnp.zeros(group.shape, jnp.float32)
    for index in range(var_ref.shape[1]):
        variance = jnp.where(group == index, var_ref[:, index : index + 1], variance)
    misfit = (predicted - observed_ref[...]) / variance
    misfit_ref[...] = misfit
    weight[...] = jnp.transpose(jnp.broadcast_to(misfit, (lanes, receptors)))
    for acc in accs:
        acc[...] = jnp.zeros(acc.shape, jnp.float32)

    def step(group, carry):
        for item in range(GROUP):
            receptor = group * GROUP + item
            scale = jnp.broadcast_to(weight[pl.ds(receptor, 1), :], (tile_rows, lanes))
            for slot in range(slots):
                start = window_start(dims, tile_ref, offset_ref, slot, receptor)
                acc = accs[(item * slots + slot) % len(accs)]
                block = foot_ref[receptor, slot].astype(jnp.float32) * scale[None]
                acc[pl.ds(start, window * tile_rows), :] += block.reshape(window * tile_rows, lanes)
        return carry

    lax.fori_loop(0, receptors // GROUP, step, 0)
    total = accs[0]
    size = tiles_y * periods * tile_rows
    chunk = 8 * tile_rows

    def finish(index, carry):
        rows = pl.ds(pl.multiple_of(index * chunk, chunk), chunk)
        value = prior_ref[rows, :]
        for acc in accs:
            value = value + acc[rows, :]
        total[rows, :] = value
        return carry

    lax.fori_loop(0, size // chunk, finish, 0)
    for dist, out in enumerate(outs):
        start = place(own ^ dist, dims)
        for row in range(lat_dev):
            out[pl.ds(row, periods, stride=lat_dev), :] = total[
                pl.ds(start + row, periods, stride=tile_rows), :
            ]


def shards(
    deviation,
    footprint,
    tile_list,
    offset,
    observed,
    obs_group,
    group_var,
    inv_time,
    inv_lat,
    inv_lon,
):
    periods, lat_dev, lon_dev = deviation.shape
    receptors, _, slots, window, tile_rows, _ = footprint.shape
    n_rec = lax.axis_size("rec")
    n_tile = lax.axis_size("tile")
    tiles_y = lat_dev * n_rec // tile_rows
    dims = (periods, tiles_y, tile_rows, lat_dev, receptors, slots, window)
    smem = pl.BlockSpec(memory_space=pltpu.SMEM)
    vmem = pl.BlockSpec(memory_space=pltpu.VMEM)
    params = pltpu.CompilerParams(vmem_limit_bytes=16 * 2**20)
    field_rows = periods * lat_dev
    block_shape = jax.ShapeDtypeStruct((field_rows, lon_dev), jnp.float32)
    line_shape = jax.ShapeDtypeStruct((1, receptors), jnp.float32)
    prior_shape = jax.ShapeDtypeStruct((tiles_y * periods * tile_rows, lon_dev), jnp.float32)
    table_shape = pltpu.VMEM(((tiles_y + 1) * periods * tile_rows, lon_dev), jnp.float32)

    def swap(value, axis, dist):
        size = lax.axis_size(axis)
        return lax.ppermute(value, axis, [(i, i ^ dist) for i in range(size)])

    local = deviation.reshape(field_rows, lon_dev)
    far = range(2, n_rec, 2)
    even = {0: local}
    for dist in far:
        even[dist] = swap(local, "rec", dist)
    blocks = []
    for dist in range(0, n_rec, 2):
        blocks += [even[dist], swap(even[dist], "rec", 1)]
    strips = [local] + [swap(local, "tile", d) for d in range(1, n_tile)]

    ones = pl.pallas_call(
        ones_kernel,
        out_shape=jax.ShapeDtypeStruct((8, lon_dev), jnp.float32),
        in_specs=[],
        out_specs=vmem,
        compiler_params=pltpu.CompilerParams(vmem_limit_bytes=2**20),
        cost_estimate=pl.CostEstimate(flops=10**10, bytes_accessed=2 * 10**7, transcendentals=0),
    )()
    tiles = tile_list[:, 0, :].T
    foot = footprint[:, 0]
    partial_pred = pl.pallas_call(
        functools.partial(forward_kernel, dims),
        out_shape=line_shape,
        in_specs=[smem] * 2 + [vmem] * (2 + n_rec),
        out_specs=vmem,
        scratch_shapes=[table_shape, pltpu.VMEM((receptors, tile_rows, lon_dev), jnp.float32)],
        compiler_params=params,
    )(tiles, offset, foot, ones, *blocks)
    preds = [partial_pred] + [swap(partial_pred, "tile", d) for d in range(1, n_tile)]
    prior = pl.pallas_call(
        functools.partial(prior_kernel, dims, n_tile),
        out_shape=prior_shape,
        in_specs=[vmem] * (n_tile + 3),
        out_specs=vmem,
        scratch_shapes=[pltpu.VMEM((field_rows, lon_dev), jnp.float32)],
        compiler_params=params,
    )(*strips, inv_lon, inv_time, inv_lat)
    results = pl.pallas_call(
        functools.partial(adjoint_kernel, dims, n_tile),
        out_shape=[block_shape] * n_rec + [line_shape],
        in_specs=[smem] * 2 + [vmem] * (n_tile + 5),
        out_specs=[vmem] * (n_rec + 1),
        scratch_shapes=[pltpu.VMEM((receptors, lon_dev), jnp.float32)] + [table_shape] * N_ACC,
        compiler_params=params,
    )(
        tiles,
        offset,
        foot,
        *preds,
        observed.reshape(1, receptors),
        obs_group.reshape(1, receptors),
        group_var.reshape(1, -1),
        prior,
    )
    misfit = results[n_rec].reshape(receptors)
    gradient = None
    for dist in list(reversed(range(2, n_rec, 2))) + [0]:
        value = results[dist] + swap(results[dist + 1], "rec", 1)
        value = value if dist == 0 else swap(value, "rec", dist)
        gradient = value if gradient is None else gradient + value
    return (gradient.reshape(periods, lat_dev, lon_dev), misfit)


def solution(mesh):
    return jax.shard_map(
        shards,
        mesh=mesh,
        in_specs=(
            P(None, "rec", "tile"),
            P("rec", "tile", None, None, None, None),
            P("rec", "tile", None),
            P("rec"),
            P("rec"),
            P("rec"),
            P(),
            P(),
            P(),
            P("tile", None),
        ),
        out_specs=(P(None, "rec", "tile"), P("rec")),
        check_vma=False,
    )
```

```python
import functools

import jax
import jax.numpy as jnp
from jax import lax
from jax.experimental import pallas as pl
from jax.experimental.pallas import tpu as pltpu
from jax.sharding import PartitionSpec as P


GROUP = 8
N_ACC = 2
HIGHEST = lax.Precision.HIGHEST


def dot(left, right, dims=((1,), (0,))):
    return lax.dot_general(
        left, right, (dims, ((), ())), precision=HIGHEST, preferred_element_type=jnp.float32
    )


def place(owner, dims):
    periods, _, tile_rows, lat_dev = dims[:4]
    row = owner * lat_dev
    return (row // tile_rows) * (periods * tile_rows) + lax.rem(row, tile_rows)


def ones_kernel(ones_ref):
    ones_ref[...] = jnp.ones(ones_ref.shape, jnp.float32)


def forward_kernel(dims, tile_ref, offset_ref, *refs):
    periods, tiles_y, tile_rows, lat_dev, receptors, slots, window = dims
    foot_ref, ones_ref, blocks = refs[0], refs[1], refs[2:-6]
    out_ref, start_ref, table, sums, mixed, sem = refs[-6:]
    lanes = table.shape[-1]
    tile = tile_ref[...]
    tile = jnp.where(tile < 0, tiles_y, tile)
    mixed[...] = (tile * periods + offset_ref[...]) * tile_rows
    copy = pltpu.make_async_copy(mixed, start_ref, sem)
    copy.start()
    own = lax.axis_index("rec")
    for dist, block in enumerate(blocks):
        start = place(own ^ dist, dims)
        for row in range(lat_dev):
            table[pl.ds(start + row, periods, stride=tile_rows), :] = block[
                pl.ds(row, periods, stride=lat_dev), :
            ]
    rest = tiles_y * periods * tile_rows
    table[pl.ds(rest, periods * tile_rows), :] = jnp.zeros((periods * tile_rows, lanes), jnp.float32)

    def step(group, carry):
        for item in range(GROUP):
            receptor = group * GROUP + item
            total = None
            for slot in range(slots):
                start = pl.multiple_of(start_ref[slot, receptor], tile_rows)
                field = table[pl.ds(start, window * tile_rows), :]
                field = field.reshape(window, tile_rows, lanes)
                block = foot_ref[receptor, slot].astype(jnp.float32)
                part = jnp.sum(block * field, axis=0)
                total = part if total is None else total + part
            sums[pl.ds(pl.multiple_of(receptor * tile_rows, tile_rows), tile_rows), :] = total
        return carry

    copy.wait()
    lax.fori_loop(0, receptors // GROUP, step, 0)
    rows = sums[pl.ds(0, receptors, stride=tile_rows), :]
    for row in range(1, tile_rows):
        rows = rows + sums[pl.ds(row, receptors, stride=tile_rows), :]
    flat = dot(ones_ref[...], rows, ((1,), (1,)))
    out_ref[...] = flat[0:1, :]


def prior_kernel(dims, n_tile, *refs):
    periods, tiles_y, tile_rows, lat_dev = dims[:4]
    own, strip = lax.axis_index("rec"), lax.axis_index("tile")
    strips = refs[:n_tile]
    lon_ref, time_ref, lat_ref, out_ref, mixed = refs[n_tile:]
    lanes = out_ref.shape[-1]
    total = None
    for dist, value in enumerate(strips):
        start = pl.multiple_of((strip ^ dist) * lanes, lanes)
        term = dot(value[...], lon_ref[:, pl.ds(start, lanes)], ((1,), (1,)))
        total = term if total is None else total + term
    mixed[...] = total
    fields = [
        dot(time_ref[...], mixed[pl.ds(row, periods, stride=lat_dev), :]) for row in range(lat_dev)
    ]
    for row in range(lat_dev):
        mixed[pl.ds(row * periods, periods), :] = fields[row]
    cols = [lat_ref[pl.ds(own * lat_dev + row, 1), :] for row in range(lat_dev)]
    cols = [
        jnp.transpose(jnp.broadcast_to(col, (lanes, col.shape[-1]))) for col in cols
    ]

    def finish(period, carry):
        lines = [
            jnp.broadcast_to(mixed[pl.ds(row * periods + period, 1), :], (tile_rows, lanes))
            for row in range(lat_dev)
        ]
        for tile in range(tiles_y):
            value = None
            for row in range(lat_dev):
                term = cols[row][tile * tile_rows : (tile + 1) * tile_rows] * lines[row]
                value = term if value is None else value + term
            start = pl.multiple_of((tile * periods + period) * tile_rows, tile_rows)
            out_ref[pl.ds(start, tile_rows), :] = value
        return carry

    lax.fori_loop(0, periods, finish, 0, unroll=8)


def adjoint_kernel(dims, n_tile, start_ref, *refs):
    periods, tiles_y, tile_rows, lat_dev, receptors, slots, window = dims
    foot_ref, refs = refs[0], refs[1:]
    preds = refs[:n_tile]
    observed_ref, group_ref, var_ref, prior_ref = refs[n_tile : n_tile + 4]
    n_rec = (tiles_y * tile_rows) // lat_dev
    outs = refs[n_tile + 4 : n_tile + 4 + n_rec]
    scratch = refs[n_tile + 4 + n_rec :]
    misfit_ref, weight = scratch[:2]
    accs = scratch[2:]
    lanes = weight.shape[-1]
    own = lax.axis_index("rec")
    predicted = preds[0][...]
    for other in preds[1:]:
        predicted = predicted + other[...]
    group = group_ref[...]
    variance = jnp.zeros(group.shape, jnp.float32)
    for index in range(var_ref.shape[1]):
        variance = jnp.where(group == index, var_ref[:, index : index + 1], variance)
    misfit = (predicted - observed_ref[...]) / variance
    misfit_ref[...] = jnp.broadcast_to(misfit, misfit_ref.shape)
    weight[...] = jnp.transpose(jnp.broadcast_to(misfit, (lanes, receptors)))
    size = tiles_y * periods * tile_rows
    for acc in accs:
        acc[pl.ds(0, size), :] = jnp.zeros((size, lanes), jnp.float32)

    def step(group, carry):
        for item in range(GROUP):
            receptor = group * GROUP + item
            scale = jnp.broadcast_to(weight[pl.ds(receptor, 1), :], (tile_rows, lanes))
            for slot in range(slots):
                start = pl.multiple_of(start_ref[slot, receptor], tile_rows)
                acc = accs[(item * slots + slot) % len(accs)]
                block = foot_ref[receptor, slot].astype(jnp.float32) * scale[None]
                acc[pl.ds(start, window * tile_rows), :] += block.reshape(window * tile_rows, lanes)
        return carry

    lax.fori_loop(0, receptors // GROUP, step, 0)
    total = accs[0]
    chunk = 8 * tile_rows

    def finish(index, carry):
        rows = pl.ds(pl.multiple_of(index * chunk, chunk), chunk)
        value = prior_ref[rows, :]
        for acc in accs:
            value = value + acc[rows, :]
        total[rows, :] = value
        return carry

    lax.fori_loop(0, size // chunk, finish, 0)
    for dist, out in enumerate(outs):
        start = place(own ^ dist, dims)
        for row in range(lat_dev):
            out[pl.ds(row, periods, stride=lat_dev), :] = total[
                pl.ds(start + row, periods, stride=tile_rows), :
            ]


def shards(
    deviation,
    footprint,
    tile_list,
    offset,
    observed,
    obs_group,
    group_var,
    inv_time,
    inv_lat,
    inv_lon,
):
    periods, lat_dev, lon_dev = deviation.shape
    receptors, _, slots, window, tile_rows, _ = footprint.shape
    n_rec = lax.axis_size("rec")
    n_tile = lax.axis_size("tile")
    tiles_y = lat_dev * n_rec // tile_rows
    dims = (periods, tiles_y, tile_rows, lat_dev, receptors, slots, window)
    smem = pl.BlockSpec(memory_space=pltpu.SMEM)
    vmem = pl.BlockSpec(memory_space=pltpu.VMEM)
    params = pltpu.CompilerParams(vmem_limit_bytes=16 * 2**20)
    field_rows = periods * lat_dev
    block_shape = jax.ShapeDtypeStruct((field_rows, lon_dev), jnp.float32)
    line_shape = jax.ShapeDtypeStruct((1, receptors), jnp.float32)
    prior_shape = jax.ShapeDtypeStruct((tiles_y * periods * tile_rows, lon_dev), jnp.float32)
    table_shape = pltpu.VMEM(((tiles_y + 1) * periods * tile_rows, lon_dev), jnp.float32)

    def swap(value, axis, dist):
        size = lax.axis_size(axis)
        return lax.ppermute(value, axis, [(i, i ^ dist) for i in range(size)])

    local = deviation.reshape(field_rows, lon_dev)
    far = range(2, n_rec, 2)
    even = {0: local}
    for dist in far:
        even[dist] = swap(local, "rec", dist)
    blocks = []
    for dist in range(0, n_rec, 2):
        blocks += [even[dist], swap(even[dist], "rec", 1)]
    strips = [local] + [swap(local, "tile", d) for d in range(1, n_tile)]

    ones = pl.pallas_call(
        ones_kernel,
        out_shape=jax.ShapeDtypeStruct((8, lon_dev), jnp.float32),
        in_specs=[],
        out_specs=vmem,
        compiler_params=pltpu.CompilerParams(vmem_limit_bytes=2**20),
        cost_estimate=pl.CostEstimate(flops=10**10, bytes_accessed=2 * 10**7, transcendentals=0),
    )()
    foot = footprint[:, 0]
    partial_pred, starts = pl.pallas_call(
        functools.partial(forward_kernel, dims),
        out_shape=[line_shape, pltpu.SMEM((slots, receptors), jnp.int32)],
        in_specs=[vmem] * (4 + n_rec),
        out_specs=[vmem, smem],
        scratch_shapes=[
            table_shape,
            pltpu.VMEM((receptors * tile_rows, lon_dev), jnp.float32),
            pltpu.VMEM((slots, receptors), jnp.int32),
            pltpu.SemaphoreType.DMA,
        ],
        compiler_params=params,
    )(tile_list[:, 0, :].T, offset.reshape(1, receptors), foot, ones, *blocks)
    preds = [partial_pred] + [swap(partial_pred, "tile", d) for d in range(1, n_tile)]
    prior = pl.pallas_call(
        functools.partial(prior_kernel, dims, n_tile),
        out_shape=prior_shape,
        in_specs=[vmem] * (n_tile + 3),
        out_specs=vmem,
        scratch_shapes=[pltpu.VMEM((field_rows, lon_dev), jnp.float32)],
        compiler_params=params,
    )(*strips, inv_lon, inv_time, inv_lat)
    results = pl.pallas_call(
        functools.partial(adjoint_kernel, dims, n_tile),
        out_shape=[block_shape] * n_rec + [jax.ShapeDtypeStruct((8, receptors), jnp.float32)],
        in_specs=[smem] + [vmem] * (n_tile + 5),
        out_specs=[vmem] * (n_rec + 1),
        scratch_shapes=[pltpu.VMEM((receptors, lon_dev), jnp.float32)] + [table_shape] * N_ACC,
        compiler_params=params,
    )(
        starts,
        foot,
        *preds,
        observed.reshape(1, receptors),
        obs_group.reshape(1, receptors),
        group_var.reshape(1, -1),
        prior,
    )
    misfit = results[n_rec][0]
    gradient = None
    for dist in list(reversed(range(2, n_rec, 2))) + [0]:
        value = results[dist] + swap(results[dist + 1], "rec", 1)
        value = value if dist == 0 else swap(value, "rec", dist)
        gradient = value if gradient is None else gradient + value
    return (gradient.reshape(periods, lat_dev, lon_dev), misfit)


def solution(mesh):
    return jax.shard_map(
        shards,
        mesh=mesh,
        in_specs=(
            P(None, "rec", "tile"),
            P("rec", "tile", None, None, None, None),
            P("rec", "tile", None),
            P("rec"),
            P("rec"),
            P("rec"),
            P(),
            P(),
            P(),
            P("tile", None),
        ),
        out_specs=(P(None, "rec", "tile"), P("rec")),
        check_vma=False,
    )
```

```python
import functools

import jax
import jax.numpy as jnp
from jax import lax
from jax.experimental import pallas as pl
from jax.experimental.pallas import tpu as pltpu
from jax.sharding import PartitionSpec as P


GROUP = 8
N_ACC = 2
HIGHEST = lax.Precision.HIGHEST


def dot(left, right, dims=((1,), (0,))):
    return lax.dot_general(
        left, right, (dims, ((), ())), precision=HIGHEST, preferred_element_type=jnp.float32
    )


def place(owner, dims):
    periods, _, tile_rows, lat_dev = dims[:4]
    row = owner * lat_dev
    return (row // tile_rows) * (periods * tile_rows) + lax.rem(row, tile_rows)


def ones_kernel(ones_ref):
    ones_ref[...] = jnp.ones(ones_ref.shape, jnp.float32)


def index_kernel(dims, tile_ref, offset_ref, start_ref, mixed, sem):
    periods, tiles_y, tile_rows = dims[:3]
    tile = tile_ref[...]
    tile = jnp.where(tile < 0, tiles_y, tile)
    mixed[...] = (tile * periods + offset_ref[...]) * tile_rows
    copy = pltpu.make_async_copy(mixed, start_ref, sem)
    copy.start()
    copy.wait()


def stack_kernel(ones_ref, *refs):
    for index, block in enumerate(refs[:-1]):
        refs[-1][index] = block[...]


def forward_kernel(dims, start_ref, foot_ref, ones_ref, even_ref, odd_ref, *refs):
    periods, tiles_y, tile_rows, lat_dev, receptors, slots, window = dims
    out_ref, table, sums = refs
    lanes = table.shape[-1]
    own = lax.axis_index("rec")
    for dist in range(2 * even_ref.shape[0]):
        block = (odd_ref if dist % 2 else even_ref).at[dist // 2]
        start = place(own ^ dist, dims)
        for row in range(lat_dev):
            table[pl.ds(start + row, periods, stride=tile_rows), :] = block[
                pl.ds(row, periods, stride=lat_dev), :
            ]
    rest = tiles_y * periods * tile_rows
    table[pl.ds(rest, periods * tile_rows), :] = jnp.zeros((periods * tile_rows, lanes), jnp.float32)

    def step(group, carry):
        for item in range(GROUP):
            receptor = group * GROUP + item
            total = None
            for slot in range(slots):
                start = pl.multiple_of(start_ref[slot, receptor], tile_rows)
                field = table[pl.ds(start, window * tile_rows), :]
                field = field.reshape(window, tile_rows, lanes)
                block = foot_ref[receptor, slot].astype(jnp.float32)
                part = jnp.sum(block * field, axis=0)
                total = part if total is None else total + part
            sums[pl.ds(pl.multiple_of(receptor * tile_rows, tile_rows), tile_rows), :] = total
        return carry

    lax.fori_loop(0, receptors // GROUP, step, 0)
    rows = sums[pl.ds(0, receptors, stride=tile_rows), :]
    for row in range(1, tile_rows):
        rows = rows + sums[pl.ds(row, receptors, stride=tile_rows), :]
    flat = dot(ones_ref[...], rows, ((1,), (1,)))
    out_ref[...] = flat[0:1, :]


def prior_kernel(dims, n_tile, *refs):
    periods, tiles_y, tile_rows, lat_dev = dims[:4]
    own, strip = lax.axis_index("rec"), lax.axis_index("tile")
    strips = refs[:n_tile]
    lon_ref, time_ref, lat_ref, out_ref, mixed = refs[n_tile:]
    lanes = out_ref.shape[-1]
    total = None
    for dist, value in enumerate(strips):
        start = pl.multiple_of((strip ^ dist) * lanes, lanes)
        term = dot(value[...], lon_ref[:, pl.ds(start, lanes)], ((1,), (1,)))
        total = term if total is None else total + term
    mixed[...] = total
    fields = [
        dot(time_ref[...], mixed[pl.ds(row, periods, stride=lat_dev), :]) for row in range(lat_dev)
    ]
    for row in range(lat_dev):
        mixed[pl.ds(row * periods, periods), :] = fields[row]
    cols = [lat_ref[pl.ds(own * lat_dev + row, 1), :] for row in range(lat_dev)]
    cols = [
        jnp.transpose(jnp.broadcast_to(col, (lanes, col.shape[-1]))) for col in cols
    ]

    def finish(period, carry):
        lines = [
            jnp.broadcast_to(mixed[pl.ds(row * periods + period, 1), :], (tile_rows, lanes))
            for row in range(lat_dev)
        ]
        for tile in range(tiles_y):
            value = None
            for row in range(lat_dev):
                term = cols[row][tile * tile_rows : (tile + 1) * tile_rows] * lines[row]
                value = term if value is None else value + term
            start = pl.multiple_of((tile * periods + period) * tile_rows, tile_rows)
            out_ref[pl.ds(start, tile_rows), :] = value
        return carry

    lax.fori_loop(0, periods, finish, 0, unroll=8)


def adjoint_kernel(dims, n_tile, start_ref, *refs):
    periods, tiles_y, tile_rows, lat_dev, receptors, slots, window = dims
    foot_ref, refs = refs[0], refs[1:]
    preds = refs[:n_tile]
    observed_ref, group_ref, var_ref, prior_ref = refs[n_tile : n_tile + 4]
    n_rec = (tiles_y * tile_rows) // lat_dev
    outs = refs[n_tile + 4 : n_tile + 4 + n_rec]
    scratch = refs[n_tile + 4 + n_rec :]
    misfit_ref, weight = scratch[:2]
    accs = scratch[2:]
    lanes = weight.shape[-1]
    own = lax.axis_index("rec")
    predicted = preds[0][...]
    for other in preds[1:]:
        predicted = predicted + other[...]
    group = group_ref[...]
    variance = jnp.zeros(group.shape, jnp.float32)
    for index in range(var_ref.shape[1]):
        variance = jnp.where(group == index, var_ref[:, index : index + 1], variance)
    misfit = (predicted - observed_ref[...]) / variance
    misfit_ref[...] = jnp.broadcast_to(misfit, misfit_ref.shape)
    weight[...] = jnp.transpose(jnp.broadcast_to(misfit, (lanes, receptors)))
    size = tiles_y * periods * tile_rows
    for acc in accs:
        acc[pl.ds(0, size), :] = jnp.zeros((size, lanes), jnp.float32)

    def step(group, carry):
        for item in range(GROUP):
            receptor = group * GROUP + item
            scale = jnp.broadcast_to(weight[pl.ds(receptor, 1), :], (tile_rows, lanes))
            for slot in range(slots):
                start = pl.multiple_of(start_ref[slot, receptor], tile_rows)
                acc = accs[(item * slots + slot) % len(accs)]
                block = foot_ref[receptor, slot].astype(jnp.float32) * scale[None]
                acc[pl.ds(start, window * tile_rows), :] += block.reshape(window * tile_rows, lanes)
        return carry

    lax.fori_loop(0, receptors // GROUP, step, 0)
    for dist, out in enumerate(outs):
        start = place(own ^ dist, dims)
        for row in range(lat_dev):
            rows = pl.ds(start + row, periods, stride=tile_rows)
            value = prior_ref[rows, :]
            for acc in accs:
                value = value + acc[rows, :]
            out[pl.ds(row, periods, stride=lat_dev), :] = value


def shards(
    deviation,
    footprint,
    tile_list,
    offset,
    observed,
    obs_group,
    group_var,
    inv_time,
    inv_lat,
    inv_lon,
):
    periods, lat_dev, lon_dev = deviation.shape
    receptors, _, slots, window, tile_rows, _ = footprint.shape
    n_rec = lax.axis_size("rec")
    n_tile = lax.axis_size("tile")
    tiles_y = lat_dev * n_rec // tile_rows
    dims = (periods, tiles_y, tile_rows, lat_dev, receptors, slots, window)
    smem = pl.BlockSpec(memory_space=pltpu.SMEM)
    vmem = pl.BlockSpec(memory_space=pltpu.VMEM)
    params = pltpu.CompilerParams(vmem_limit_bytes=16 * 2**20)
    field_rows = periods * lat_dev
    block_shape = jax.ShapeDtypeStruct((field_rows, lon_dev), jnp.float32)
    line_shape = jax.ShapeDtypeStruct((1, receptors), jnp.float32)
    prior_shape = jax.ShapeDtypeStruct((tiles_y * periods * tile_rows, lon_dev), jnp.float32)
    table_shape = pltpu.VMEM(((tiles_y + 1) * periods * tile_rows, lon_dev), jnp.float32)

    def swap(value, axis, dist):
        size = lax.axis_size(axis)
        return lax.ppermute(value, axis, [(i, i ^ dist) for i in range(size)])

    local = deviation.reshape(field_rows, lon_dev)
    even = [local] + [swap(local, "rec", dist) for dist in range(2, n_rec, 2)]
    ones = pl.pallas_call(
        ones_kernel,
        out_shape=jax.ShapeDtypeStruct((8, lon_dev), jnp.float32),
        in_specs=[],
        out_specs=vmem,
        compiler_params=pltpu.CompilerParams(vmem_limit_bytes=2**20),
        cost_estimate=pl.CostEstimate(flops=10**10, bytes_accessed=2 * 10**7, transcendentals=0),
    )()
    even = pl.pallas_call(
        stack_kernel,
        out_shape=jax.ShapeDtypeStruct((n_rec // 2, field_rows, lon_dev), jnp.float32),
        in_specs=[vmem] * (n_rec // 2 + 1),
        out_specs=vmem,
        compiler_params=pltpu.CompilerParams(vmem_limit_bytes=8 * 2**20),
    )(ones, *even)
    odd = swap(even, "rec", 1)
    strips = [local] + [swap(local, "tile", d) for d in range(1, n_tile)]

    foot = footprint[:, 0]
    starts = pl.pallas_call(
        functools.partial(index_kernel, dims),
        out_shape=pltpu.SMEM((slots, receptors), jnp.int32),
        in_specs=[vmem] * 2,
        out_specs=smem,
        scratch_shapes=[pltpu.VMEM((slots, receptors), jnp.int32), pltpu.SemaphoreType.DMA],
        compiler_params=pltpu.CompilerParams(vmem_limit_bytes=2**20),
    )(tile_list[:, 0, :].T, offset.reshape(1, receptors))
    partial_pred = pl.pallas_call(
        functools.partial(forward_kernel, dims),
        out_shape=line_shape,
        in_specs=[smem] + [vmem] * 4,
        out_specs=vmem,
        scratch_shapes=[
            table_shape,
            pltpu.VMEM((receptors * tile_rows, lon_dev), jnp.float32),
        ],
        compiler_params=params,
    )(starts, foot, ones, even, odd)
    preds = [partial_pred] + [swap(partial_pred, "tile", d) for d in range(1, n_tile)]
    prior = pl.pallas_call(
        functools.partial(prior_kernel, dims, n_tile),
        out_shape=prior_shape,
        in_specs=[vmem] * (n_tile + 3),
        out_specs=vmem,
        scratch_shapes=[pltpu.VMEM((field_rows, lon_dev), jnp.float32)],
        compiler_params=params,
    )(*strips, inv_lon, inv_time, inv_lat)
    results = pl.pallas_call(
        functools.partial(adjoint_kernel, dims, n_tile),
        out_shape=[block_shape] * n_rec + [jax.ShapeDtypeStruct((8, receptors), jnp.float32)],
        in_specs=[smem] + [vmem] * (n_tile + 5),
        out_specs=[vmem] * (n_rec + 1),
        scratch_shapes=[pltpu.VMEM((receptors, lon_dev), jnp.float32)] + [table_shape] * N_ACC,
        compiler_params=params,
    )(
        starts,
        foot,
        *preds,
        observed.reshape(1, receptors),
        obs_group.reshape(1, receptors),
        group_var.reshape(1, -1),
        prior,
    )
    misfit = results[n_rec][0]
    gradient = None
    for dist in list(reversed(range(2, n_rec, 2))) + [0]:
        value = results[dist] + swap(results[dist + 1], "rec", 1)
        value = value if dist == 0 else swap(value, "rec", dist)
        gradient = value if gradient is None else gradient + value
    return (gradient.reshape(periods, lat_dev, lon_dev), misfit)


def solution(mesh):
    return jax.shard_map(
        shards,
        mesh=mesh,
        in_specs=(
            P(None, "rec", "tile"),
            P("rec", "tile", None, None, None, None),
            P("rec", "tile", None),
            P("rec"),
            P("rec"),
            P("rec"),
            P(),
            P(),
            P(),
            P("tile", None),
        ),
        out_specs=(P(None, "rec", "tile"), P("rec")),
        check_vma=False,
    )
```

```python
import functools

import jax
import jax.numpy as jnp
from jax import lax
from jax.experimental import pallas as pl
from jax.experimental.pallas import tpu as pltpu
from jax.sharding import PartitionSpec as P


GROUP = 8
N_ACC = 2
HIGHEST = lax.Precision.HIGHEST


def dot(left, right, dims=((1,), (0,))):
    return lax.dot_general(
        left, right, (dims, ((), ())), precision=HIGHEST, preferred_element_type=jnp.float32
    )


def place(owner, dims):
    periods, _, tile_rows, lat_dev = dims[:4]
    row = owner * lat_dev
    return (row // tile_rows) * (periods * tile_rows) + lax.rem(row, tile_rows)


def ones_kernel(ones_ref):
    ones_ref[...] = jnp.ones(ones_ref.shape, jnp.float32)


def index_kernel(dims, tile_ref, offset_ref, start_ref, mixed, sem):
    periods, tiles_y, tile_rows = dims[:3]
    tile = tile_ref[...]
    tile = jnp.where(tile < 0, tiles_y, tile)
    mixed[...] = (tile * periods + offset_ref[...]) * tile_rows
    copy = pltpu.make_async_copy(mixed, start_ref, sem)
    copy.start()
    copy.wait()


def stack_kernel(ones_ref, *refs):
    for index, block in enumerate(refs[:-1]):
        refs[-1][index] = block[...]


def forward_kernel(dims, start_ref, foot_ref, even_ref, odd_ref, *refs):
    periods, tiles_y, tile_rows, lat_dev, receptors, slots, window = dims
    out_ref, table, sums = refs
    lanes = table.shape[-1]
    own = lax.axis_index("rec")
    for dist in range(2 * even_ref.shape[0]):
        block = (odd_ref if dist % 2 else even_ref).at[dist // 2]
        start = place(own ^ dist, dims)
        for row in range(lat_dev):
            table[pl.ds(start + row, periods, stride=tile_rows), :] = block[
                pl.ds(row, periods, stride=lat_dev), :
            ]
    rest = tiles_y * periods * tile_rows
    table[pl.ds(rest, periods * tile_rows), :] = jnp.zeros((periods * tile_rows, lanes), jnp.float32)

    def step(group, carry):
        for item in range(GROUP):
            receptor = group * GROUP + item
            total = None
            for slot in range(slots):
                start = pl.multiple_of(start_ref[slot, receptor], tile_rows)
                field = table[pl.ds(start, window * tile_rows), :]
                field = field.reshape(window, tile_rows, lanes)
                block = foot_ref[receptor, slot].astype(jnp.float32)
                part = jnp.sum(block * field, axis=0)
                total = part if total is None else total + part
            sums[pl.ds(pl.multiple_of(receptor * tile_rows, tile_rows), tile_rows), :] = total
        return carry

    lax.fori_loop(0, receptors // GROUP, step, 0)
    rows = sums[pl.ds(0, receptors, stride=tile_rows), :]
    for row in range(1, tile_rows):
        rows = rows + sums[pl.ds(row, receptors, stride=tile_rows), :]
    out_ref[...] = jnp.sum(jnp.transpose(rows), axis=0, keepdims=True)


def prior_kernel(dims, n_tile, *refs):
    periods, tiles_y, tile_rows, lat_dev = dims[:4]
    own, strip = lax.axis_index("rec"), lax.axis_index("tile")
    strips = refs[:n_tile]
    lon_ref, time_ref, lat_ref, out_ref, mixed = refs[n_tile:]
    lanes = out_ref.shape[-1]
    total = None
    for dist, value in enumerate(strips):
        start = pl.multiple_of((strip ^ dist) * lanes, lanes)
        term = dot(value[...], lon_ref[:, pl.ds(start, lanes)], ((1,), (1,)))
        total = term if total is None else total + term
    mixed[...] = total
    fields = [
        dot(time_ref[...], mixed[pl.ds(row, periods, stride=lat_dev), :]) for row in range(lat_dev)
    ]
    for row in range(lat_dev):
        mixed[pl.ds(row * periods, periods), :] = fields[row]
    cols = [lat_ref[pl.ds(own * lat_dev + row, 1), :] for row in range(lat_dev)]
    cols = [
        jnp.transpose(jnp.broadcast_to(col, (lanes, col.shape[-1]))) for col in cols
    ]

    def finish(period, carry):
        lines = [
            jnp.broadcast_to(mixed[pl.ds(row * periods + period, 1), :], (tile_rows, lanes))
            for row in range(lat_dev)
        ]
        for tile in range(tiles_y):
            value = None
            for row in range(lat_dev):
                term = cols[row][tile * tile_rows : (tile + 1) * tile_rows] * lines[row]
                value = term if value is None else value + term
            start = pl.multiple_of((tile * periods + period) * tile_rows, tile_rows)
            out_ref[pl.ds(start, tile_rows), :] = value
        return carry

    lax.fori_loop(0, periods, finish, 0, unroll=8)


def adjoint_kernel(dims, n_tile, start_ref, *refs):
    periods, tiles_y, tile_rows, lat_dev, receptors, slots, window = dims
    foot_ref, refs = refs[0], refs[1:]
    preds = refs[:n_tile]
    observed_ref, group_ref, var_ref, prior_ref = refs[n_tile : n_tile + 4]
    n_rec = (tiles_y * tile_rows) // lat_dev
    outs = refs[n_tile + 4 : n_tile + 4 + n_rec]
    scratch = refs[n_tile + 4 + n_rec :]
    misfit_ref, weight = scratch[:2]
    accs = scratch[2:]
    lanes = weight.shape[-1]
    own = lax.axis_index("rec")
    predicted = preds[0][...]
    for other in preds[1:]:
        predicted = predicted + other[...]
    group = group_ref[...]
    variance = jnp.zeros(group.shape, jnp.float32)
    for index in range(var_ref.shape[1]):
        variance = jnp.where(group == index, var_ref[:, index : index + 1], variance)
    misfit = (predicted - observed_ref[...]) / variance
    misfit_ref[...] = jnp.broadcast_to(misfit, misfit_ref.shape)
    weight[...] = jnp.transpose(jnp.broadcast_to(misfit, (lanes, receptors)))
    size = tiles_y * periods * tile_rows
    for acc in accs:
        acc[pl.ds(0, size), :] = jnp.zeros((size, lanes), jnp.float32)

    def step(group, carry):
        for item in range(GROUP):
            receptor = group * GROUP + item
            scale = jnp.broadcast_to(weight[pl.ds(receptor, 1), :], (tile_rows, lanes))
            for slot in range(slots):
                start = pl.multiple_of(start_ref[slot, receptor], tile_rows)
                acc = accs[(item * slots + slot) % len(accs)]
                block = foot_ref[receptor, slot].astype(jnp.float32) * scale[None]
                acc[pl.ds(start, window * tile_rows), :] += block.reshape(window * tile_rows, lanes)
        return carry

    lax.fori_loop(0, receptors // GROUP, step, 0)
    for dist, out in enumerate(outs):
        start = place(own ^ dist, dims)
        for row in range(lat_dev):
            rows = pl.ds(start + row, periods, stride=tile_rows)
            value = prior_ref[rows, :]
            for acc in accs:
                value = value + acc[rows, :]
            out[pl.ds(row, periods, stride=lat_dev), :] = value


def shards(
    deviation,
    footprint,
    tile_list,
    offset,
    observed,
    obs_group,
    group_var,
    inv_time,
    inv_lat,
    inv_lon,
):
    periods, lat_dev, lon_dev = deviation.shape
    receptors, _, slots, window, tile_rows, _ = footprint.shape
    n_rec = lax.axis_size("rec")
    n_tile = lax.axis_size("tile")
    tiles_y = lat_dev * n_rec // tile_rows
    dims = (periods, tiles_y, tile_rows, lat_dev, receptors, slots, window)
    smem = pl.BlockSpec(memory_space=pltpu.SMEM)
    vmem = pl.BlockSpec(memory_space=pltpu.VMEM)
    params = pltpu.CompilerParams(vmem_limit_bytes=16 * 2**20)
    field_rows = periods * lat_dev
    block_shape = jax.ShapeDtypeStruct((field_rows, lon_dev), jnp.float32)
    line_shape = jax.ShapeDtypeStruct((1, receptors), jnp.float32)
    prior_shape = jax.ShapeDtypeStruct((tiles_y * periods * tile_rows, lon_dev), jnp.float32)
    table_shape = pltpu.VMEM(((tiles_y + 1) * periods * tile_rows, lon_dev), jnp.float32)

    def swap(value, axis, dist):
        size = lax.axis_size(axis)
        return lax.ppermute(value, axis, [(i, i ^ dist) for i in range(size)])

    local = deviation.reshape(field_rows, lon_dev)
    even = [local] + [swap(local, "rec", dist) for dist in range(2, n_rec, 2)]
    ones = pl.pallas_call(
        ones_kernel,
        out_shape=jax.ShapeDtypeStruct((8, lon_dev), jnp.float32),
        in_specs=[],
        out_specs=vmem,
        compiler_params=pltpu.CompilerParams(vmem_limit_bytes=2**20),
        cost_estimate=pl.CostEstimate(flops=10**10, bytes_accessed=2 * 10**7, transcendentals=0),
    )()
    even = pl.pallas_call(
        stack_kernel,
        out_shape=jax.ShapeDtypeStruct((n_rec // 2, field_rows, lon_dev), jnp.float32),
        in_specs=[vmem] * (n_rec // 2 + 1),
        out_specs=vmem,
        compiler_params=pltpu.CompilerParams(vmem_limit_bytes=8 * 2**20),
    )(ones, *even)
    odd = swap(even, "rec", 1)
    strips = [local] + [swap(local, "tile", d) for d in range(1, n_tile)]

    foot = footprint[:, 0]
    starts = pl.pallas_call(
        functools.partial(index_kernel, dims),
        out_shape=pltpu.SMEM((slots, receptors), jnp.int32),
        in_specs=[vmem] * 2,
        out_specs=smem,
        scratch_shapes=[pltpu.VMEM((slots, receptors), jnp.int32), pltpu.SemaphoreType.DMA],
        compiler_params=pltpu.CompilerParams(vmem_limit_bytes=2**20),
    )(tile_list[:, 0, :].T, offset.reshape(1, receptors))
    partial_pred = pl.pallas_call(
        functools.partial(forward_kernel, dims),
        out_shape=line_shape,
        in_specs=[smem] + [vmem] * 3,
        out_specs=vmem,
        scratch_shapes=[
            table_shape,
            pltpu.VMEM((receptors * tile_rows, lon_dev), jnp.float32),
        ],
        compiler_params=params,
    )(starts, foot, even, odd)
    preds = [partial_pred] + [swap(partial_pred, "tile", d) for d in range(1, n_tile)]
    prior = pl.pallas_call(
        functools.partial(prior_kernel, dims, n_tile),
        out_shape=prior_shape,
        in_specs=[vmem] * (n_tile + 3),
        out_specs=vmem,
        scratch_shapes=[pltpu.VMEM((field_rows, lon_dev), jnp.float32)],
        compiler_params=params,
    )(*strips, inv_lon, inv_time, inv_lat)
    results = pl.pallas_call(
        functools.partial(adjoint_kernel, dims, n_tile),
        out_shape=[block_shape] * n_rec + [jax.ShapeDtypeStruct((8, receptors), jnp.float32)],
        in_specs=[smem] + [vmem] * (n_tile + 5),
        out_specs=[vmem] * (n_rec + 1),
        scratch_shapes=[pltpu.VMEM((receptors, lon_dev), jnp.float32)] + [table_shape] * N_ACC,
        compiler_params=params,
    )(
        starts,
        foot,
        *preds,
        observed.reshape(1, receptors),
        obs_group.reshape(1, receptors),
        group_var.reshape(1, -1),
        prior,
    )
    misfit = results[n_rec][0]
    gradient = None
    for dist in list(reversed(range(2, n_rec, 2))) + [0]:
        value = results[dist] + swap(results[dist + 1], "rec", 1)
        value = value if dist == 0 else swap(value, "rec", dist)
        gradient = value if gradient is None else gradient + value
    return (gradient.reshape(periods, lat_dev, lon_dev), misfit)


def solution(mesh):
    return jax.shard_map(
        shards,
        mesh=mesh,
        in_specs=(
            P(None, "rec", "tile"),
            P("rec", "tile", None, None, None, None),
            P("rec", "tile", None),
            P("rec"),
            P("rec"),
            P("rec"),
            P(),
            P(),
            P(),
            P("tile", None),
        ),
        out_specs=(P(None, "rec", "tile"), P("rec")),
        check_vma=False,
    )
```
